32 devices in a mesh: task: 4 (over x, core), param: 8 (over z, y).
Axes of the slice: x: 2, y: 2, z: 4, core: 2. Of those that a mesh axis runs over, the one named last changes fastest.
Arguments:
- acts: bfloat16 [128, 3584], replicated, may hold values from -6 to 6
- out_grads: bfloat16 [4, 128, 10240], P('task', None, 'param'), may hold values from -12 to 12
- order: int32 [4], replicated, may hold values from 0 to 3, each once
Outputs:
- update: float32 [3584, 10240], P('task', 'param')
- weights: float32 [4], replicated
The draws below stay inside these ranges and needn't reach their ends.
All inputs are finite; a program needn't handle non-finite values.
Results may differ from the reference program's by a relative error of at most 0.0029.
Values may be sent and summed in bfloat16 or wider, within the bound.
A program may use at most 64 MiB of HBM per device.

```python
import jax
import jax.numpy as jnp
from jax import lax

D = 3584
FFW = 10240
TOK = 128
TASKS = 4
N_PARAM = 8


def draw_out_grads(key, part):
    keys = jax.random.split(jax.random.fold_in(key, 17), 7)
    shared = jnp.clip(jax.random.normal(keys[0], (TOK, FFW), jnp.float32), -4.5, 4.5)
    base = jax.random.uniform(keys[1], (TASKS, 1, 1), jnp.float32, -1.2, 1.2)
    vary = jax.random.uniform(keys[2], (TASKS, 1, 16), jnp.float32, -0.8, 0.8)
    block_ids = jnp.arange(FFW, dtype=jnp.int32) * 16 // FFW
    coupling = base + jnp.take(vary, block_ids, axis=2)
    task_scale = jnp.exp(jax.random.uniform(keys[3], (TASKS, 1, 1), jnp.float32, jnp.log(0.5), jnp.log(2.0)))
    common_col = jnp.exp(jax.random.uniform(keys[4], (1, 1, FFW), jnp.float32, jnp.log(0.3), jnp.log(3.0)))
    own_col = jnp.exp(jax.random.uniform(keys[5], (TASKS, 1, FFW), jnp.float32, jnp.log(0.2), jnp.log(5.0)))
    noise = jnp.clip(jax.random.normal(keys[6], (TASKS, TOK, FFW), jnp.float32), -5.0, 5.0)
    values = task_scale * common_col * own_col * (coupling * shared[None] + noise) / jnp.sqrt(TOK * 1.0)
    return jnp.clip(values, -12.0, 12.0).astype(jnp.bfloat16)


def normal_values(rng, shape, scale, bound, kind=jnp.bfloat16):
    return jnp.clip(scale * jax.random.normal(rng, shape, jnp.float32), -bound, bound).astype(kind)


def setup_inputs(seed: int = 0) -> dict:
    seeds = jax.random.split(jax.random.key(seed), 4)
    acts = normal_values(seeds[0], (TOK, D), 1.0, 6.0)
    out_grads = draw_out_grads(jax.random.fold_in(seeds[3], 71), 0)
    order = jax.random.permutation(seeds[2], TASKS).astype(jnp.int32)
    return dict(acts=acts, out_grads=out_grads, order=order)


def pcgrad_weights(gram, order):
    count = gram.shape[0]
    ids = jnp.arange(count, dtype=jnp.int32)

    def turn(step, mix):
        target = order[step]
        column = gram[:, target]
        onehot = (ids == target).astype(jnp.float32)
        dots = jnp.dot(mix, column, precision=lax.Precision.HIGHEST)
        scale = jnp.sum(column * onehot) + 1e-6
        change = jnp.minimum(dots, 0.0) / scale * (1.0 - onehot)
        return mix - change[:, None] * onehot[None, :]

    mix = lax.fori_loop(0, count, turn, jnp.eye(count, dtype=jnp.float32))
    return jnp.sum(mix, axis=0)


def reference(acts, out_grads, order):
    tasks, tokens, width = out_grads.shape
    block = FFW // N_PARAM
    stacked = out_grads.reshape(tasks, tokens, width // block, block).transpose(2, 0, 1, 3)

    def add(gram, part):
        grads = jnp.einsum("td,ktc->kdc", acts.astype(jnp.float32), part.astype(jnp.float32)).astype(jnp.bfloat16)
        flat = grads.reshape(tasks, -1)
        return gram + jnp.dot(flat, flat.T, preferred_element_type=jnp.float32), None

    gram, _ = lax.scan(add, jnp.zeros((tasks, tasks), jnp.float32), stacked)
    weights = pcgrad_weights(gram, order)
    combined = jnp.einsum("k,ktc->tc", weights, out_grads.astype(jnp.float32), precision=lax.Precision.HIGHEST).astype(jnp.bfloat16)
    update = jnp.dot(acts.T, combined, preferred_element_type=jnp.float32)
    return (update, weights)
```

```python
import functools

import jax
import jax.numpy as jnp
from jax import lax
from jax.experimental import pallas as pl
from jax.experimental.pallas import tpu as pltpu
from jax.sharding import PartitionSpec as P

MESH = pl.DeviceIdType.MESH
LANES = 128


def task_device(index):
    return {"task": index}


def column_blocks(columns, groups):
    tiles = columns // LANES
    edges = [tiles * g // groups for g in range(groups + 1)]
    return [(edges[g] * LANES, (edges[g + 1] - edges[g]) * LANES) for g in range(groups)]


def pcgrad_weights(gram_row, order_ref, tasks):
    rows = max(8, tasks)
    sub = lax.broadcasted_iota(jnp.int32, (rows, LANES), 0)
    lane = lax.broadcasted_iota(jnp.int32, (rows, LANES), 1)
    flat = jnp.broadcast_to(gram_row, (rows, LANES))
    targets, columns, scales = [], [], []
    for step in range(tasks):
        target = order_ref[step]
        column = jnp.sum(jnp.where(lane == sub * tasks + target, flat, 0.0), axis=1, keepdims=True)
        scale = jnp.sum(jnp.where(lane == target * (tasks + 1), flat, 0.0), axis=1, keepdims=True)
        targets.append(target)
        columns.append(jnp.broadcast_to(column, (rows, LANES)))
        scales.append(scale[:1] + 1e-6)
    mix = jnp.where((sub == lane) & (sub < tasks), 1.0, 0.0)
    for target, column, scale in zip(targets, columns, scales):
        dots = jnp.sum(mix * column, axis=0, keepdims=True)
        change = jnp.minimum(dots, 0.0) / scale
        mix = mix - jnp.where((sub == target) & (lane != target), change, 0.0)
    return jnp.sum(mix, axis=1, keepdims=True)


def mixer(
    groups,
    others,
    order_ref,
    acts_hbm,
    grads_hbm,
    combined_ref,
    weights_ref,
    acts_v,
    every,
    kernel_mat,
    rows_ref,
    mine_ref,
    gath,
    local_sem,
    send_sem,
    near_recv,
    far_recv,
    fwd_send,
    fwd_recv,
    row_send,
    row_recv,
):
    me = lax.axis_index("task")
    place = lax.axis_index("param")
    core = lax.rem(me, 2)
    partner = me + 1 - 2 * core
    total = groups * others
    chips = groups // 2
    chip = me // 2
    linear = me * others + place
    tokens, columns = every.shape[1:]
    blocks = column_blocks(columns, groups)
    live = [index for index in range(groups) if blocks[index][1] > 0]

    load_grads = pltpu.make_async_copy(grads_hbm.at[0], every.at[me], local_sem.at[0])
    load_acts = pltpu.make_async_copy(acts_hbm, acts_v, local_sem.at[1])
    load_grads.start()
    load_acts.start()

    def device(index):
        return {"task": index // others, "param": lax.rem(index, others)}

    barrier = pltpu.get_barrier_semaphore()

    @pl.loop(1, total)
    def _(step):
        pl.semaphore_signal(
            barrier, inc=1, device_id=device(lax.rem(linear + step, total)), device_id_type=MESH
        )

    load_acts.wait()
    acts = acts_v[...]
    outer = lax.dot_general(acts, acts, (((1,), (1,)), ((), ())), preferred_element_type=jnp.float32)
    high = outer.astype(jnp.bfloat16)
    rest = outer - high.astype(jnp.float32)
    mid = rest.astype(jnp.bfloat16)
    low = (rest - mid.astype(jnp.float32)).astype(jnp.bfloat16)
    kernel_mat[0:tokens] = high
    kernel_mat[tokens : 2 * tokens] = mid
    kernel_mat[2 * tokens :] = low
    load_grads.wait()
    pl.semaphore_wait(barrier, total - 1)

    def block(task, index):
        start, size = blocks[index]
        return every.at[task, :, pl.ds(start, size)]

    def send(index, target, slot, recv):
        return pltpu.make_async_remote_copy(
            src_ref=block(me, index),
            dst_ref=block(me, index),
            send_sem=send_sem.at[slot, index],
            recv_sem=recv,
            device_id={"task": target},
            device_id_type=MESH,
        )

    across = pltpu.make_async_remote_copy(
        src_ref=every.at[me],
        dst_ref=every.at[me],
        send_sem=send_sem.at[0, 0],
        recv_sem=near_recv.at[me],
        device_id={"task": partner},
        device_id_type=MESH,
    )
    across.start()

    sends = []
    for hop in range(1, chips):
        for index in live:
            other = lax.rem(chip + hop, chips)
            target = other * 2 + index % 2
            first = other == index // 2

            @pl.when(first)
            def _():
                send(index, target, hop, near_recv.at[me]).start()

    for hop in range(1, chips):
        for index in live:
            other = lax.rem(chip + hop, chips)
            target = other * 2 + index % 2
            first = other == index // 2

            @pl.when(jnp.logical_not(first))
            def _():
                send(index, target, hop, far_recv.at[me, index]).start()

    def forward(task, index):
        return pltpu.make_async_remote_copy(
            src_ref=block(task, index),
            dst_ref=block(task, index),
            send_sem=fwd_send.at[task, index],
            recv_sem=fwd_recv.at[task, index],
            device_id={"task": partner},
            device_id_type=MESH,
        )

    def waiter(ref, sem):
        return pltpu.make_async_copy(ref, ref, sem)

    waiter(every.at[partner], near_recv.at[partner]).wait()
    for hop in range(1, chips):
        for source_core in range(2):
            task = lax.rem(chip + hop, chips) * 2 + source_core
            for index in live:

                @pl.when(me == index)
                def _():
                    waiter(block(task, index), near_recv.at[task]).wait()
                    forward(task, index).start()

    tiles = columns // LANES
    first_tile = (tiles * me) // groups
    count = (tiles * (me + 1)) // groups - first_tile
    sizes = [size // LANES for _, size in blocks]
    rows_ref[...] = jnp.zeros_like(rows_ref)
    pairs = [(i, j) for i in range(groups) for j in range(i, groups)]

    def share(slot):
        at = pl.multiple_of((first_tile + slot) * LANES, LANES)
        parts = [every[k, :, pl.ds(at, LANES)] for k in range(groups)]
        weighted = []
        for part in parts:
            wide = jnp.dot(kernel_mat[...], part, preferred_element_type=jnp.float32)
            weighted.append(wide[:tokens] + (wide[tokens : 2 * tokens] + wide[2 * tokens :]))
        plain = [part.astype(jnp.float32) for part in parts]
        for i, j in pairs:
            row = jnp.sum(weighted[i] * plain[j], axis=0, keepdims=True)
            spot = i * groups + j
            rows_ref[spot : spot + 1, :] += row
            if i != j:
                spot = j * groups + i
                rows_ref[spot : spot + 1, :] += row

    for slot in range(max(sizes)):
        if slot < min(sizes):
            share(slot)
        else:
            pl.when(count > slot)(functools.partial(share, slot))

    entries = groups * groups
    sums = jnp.sum(rows_ref[...], axis=1, keepdims=True)
    sub = lax.broadcasted_iota(jnp.int32, (entries, LANES), 0)
    lane = lax.broadcasted_iota(jnp.int32, (entries, LANES), 1)
    row = jnp.sum(jnp.where(sub == lane, sums, 0.0), axis=0, keepdims=True)
    mine_ref[...] = row
    gath[linear] = row

    @pl.loop(1, total)
    def _(step):
        pltpu.make_async_remote_copy(
            src_ref=mine_ref,
            dst_ref=gath.at[linear],
            send_sem=row_send,
            recv_sem=row_recv,
            device_id=device(lax.rem(linear + step, total)),
            device_id_type=MESH,
        ).start()

    for hop in range(1, chips):
        other = lax.rem(chip + hop, chips)
        for index in live:
            for source_core in range(2):
                task = other * 2 + source_core

                @pl.when((chip != index // 2) & (core == index % 2))
                def _():
                    waiter(block(task, index), far_recv.at[task, index]).wait()
                    forward(task, index).start()

    for hop in range(1, chips):
        other = lax.rem(chip + hop, chips)
        for index in live:
            for source_core in range(2):
                task = other * 2 + source_core

                @pl.when(core != index % 2)
                def _():
                    waiter(block(task, index), fwd_recv.at[task, index]).wait()

    bulk = gath.at[pl.ds(0, total - 1)]
    waiter(bulk, row_recv).wait()
    gram_row = jnp.sum(gath[...], axis=0)
    weights = pcgrad_weights(gram_row, order_ref, groups)

    @pl.loop(0, tiles)
    def _(tile):
        at = pl.ds(pl.multiple_of(tile * LANES, LANES), LANES)
        mixed = weights[0:1] * every[0, :, at].astype(jnp.float32)
        for k in range(1, groups):
            mixed = mixed + weights[k : k + 1] * every[k, :, at].astype(jnp.float32)
        combined_ref[:, at] = mixed.astype(jnp.bfloat16)

    weights_ref[...] = jnp.broadcast_to(weights, weights_ref.shape)

    waiter(bulk, row_send).wait()
    waiter(every.at[me], send_sem.at[0, 0]).wait()
    for hop in range(1, chips):
        other = lax.rem(chip + hop, chips)
        for index in live:
            waiter(block(me, index), send_sem.at[hop, index]).wait()
            for source_core in range(2):
                task = other * 2 + source_core

                @pl.when(core == index % 2)
                def _():
                    waiter(block(task, index), fwd_send.at[task, index]).wait()


def shards(acts, out_grads, order):
    groups = lax.axis_size("task")
    others = lax.axis_size("param")
    total = groups * others
    tokens, columns = out_grads.shape[1:]
    part_rows = acts.shape[1] // groups
    dma = pltpu.SemaphoreType.DMA
    combined, weights = pl.pallas_call(
        functools.partial(mixer, groups, others),
        out_shape=(
            jax.ShapeDtypeStruct((tokens, columns), jnp.bfloat16),
            jax.ShapeDtypeStruct((max(8, groups), LANES), jnp.float32),
        ),
        in_specs=[
            pl.BlockSpec(memory_space=pltpu.SMEM),
            pl.BlockSpec(memory_space=pl.ANY),
            pl.BlockSpec(memory_space=pl.ANY),
        ],
        out_specs=(
            pl.BlockSpec(memory_space=pltpu.VMEM),
            pl.BlockSpec(memory_space=pltpu.VMEM),
        ),
        scratch_shapes=[
            pltpu.VMEM(acts.shape, jnp.bfloat16),
            pltpu.VMEM((groups, tokens, columns), jnp.bfloat16),
            pltpu.VMEM((3 * tokens, tokens), jnp.bfloat16),
            pltpu.VMEM((groups * groups, LANES), jnp.float32),
            pltpu.VMEM((1, LANES), jnp.float32),
            pltpu.VMEM((total, 1, LANES), jnp.float32),
            dma((2,)),
            dma((groups, groups)),
            dma((groups,)),
            dma((groups, groups)),
            dma((groups, groups)),
            dma((groups, groups)),
            dma,
            dma,
        ],
        compiler_params=pltpu.CompilerParams(collective_id=0, has_side_effects=True),
        name="mixer",
    )(order, acts, out_grads)
    group_id = lax.axis_index("task")
    acts_rows = lax.dynamic_slice_in_dim(acts, group_id * part_rows, part_rows, 1)
    update = lax.dot_general(
        acts_rows, combined, (((0,), (0,)), ((), ())), preferred_element_type=jnp.float32
    )
    return (update, weights[:groups, 0])


def solution(mesh):
    in_specs = (P(), P("task", None, "param"), P())
    out_specs = (P("task", "param"), P())
    return jax.shard_map(shards, mesh=mesh, in_specs=in_specs, out_specs=out_specs, check_vma=False)
```

```python
import functools

import jax
import jax.numpy as jnp
from jax import lax
from jax.experimental import pallas as pl
from jax.experimental.pallas import tpu as pltpu
from jax.sharding import PartitionSpec as P

MESH = pl.DeviceIdType.MESH
LANES = 128
VMEM_BYTES = 67043328


def column_blocks(columns, groups):
    tiles = columns // LANES
    edges = [tiles * g // groups for g in range(groups + 1)]
    return [(edges[g] * LANES, (edges[g + 1] - edges[g]) * LANES) for g in range(groups)]


def pcgrad_weights(gram_row, order_ref, tasks):
    rows = max(8, tasks)
    sub = lax.broadcasted_iota(jnp.int32, (rows, LANES), 0)
    lane = lax.broadcasted_iota(jnp.int32, (rows, LANES), 1)
    flat = jnp.broadcast_to(gram_row, (rows, LANES))
    targets, columns, scales = [], [], []
    for step in range(tasks):
        target = order_ref[step]
        column = jnp.sum(jnp.where(lane == sub * tasks + target, flat, 0.0), axis=1, keepdims=True)
        scale = jnp.sum(jnp.where(lane == target * (tasks + 1), flat, 0.0), axis=1, keepdims=True)
        targets.append(target)
        columns.append(jnp.broadcast_to(column, (rows, LANES)))
        scales.append(scale[:1] + 1e-6)
    mix = jnp.where((sub == lane) & (sub < tasks), 1.0, 0.0)
    for target, column, scale in zip(targets, columns, scales):
        dots = jnp.sum(mix * column, axis=0, keepdims=True)
        change = jnp.minimum(dots, 0.0) / scale
        mix = mix - jnp.where((sub == target) & (lane != target), change, 0.0)
    return jnp.sum(mix, axis=1, keepdims=True)


def mixer(
    groups,
    others,
    order_ref,
    acts_hbm,
    grads_hbm,
    combined_ref,
    acts_t,
    weights_ref,
    acts_v,
    every,
    kernel_mat,
    own_prod,
    partner_prod,
    rows_ref,
    turned,
    mine_ref,
    gath,
    local_sem,
    send_sem,
    near_recv,
    far_recv,
    fwd_send,
    fwd_recv,
    row_send,
    row_recv,
):
    me = lax.axis_index("task")
    place = lax.axis_index("param")
    core = lax.rem(me, 2)
    partner = me + 1 - 2 * core
    total = groups * others
    chips = groups // 2
    chip = me // 2
    linear = me * others + place
    tokens, columns = every.shape[1:]
    blocks = column_blocks(columns, groups)
    live = [index for index in range(groups) if blocks[index][1] > 0]

    load_grads = pltpu.make_async_copy(grads_hbm.at[0], every.at[me], local_sem.at[0])
    load_acts = pltpu.make_async_copy(acts_hbm, acts_v, local_sem.at[1])
    load_grads.start()
    load_acts.start()

    def device(index):
        return {"task": index // others, "param": lax.rem(index, others)}

    barrier = pltpu.get_barrier_semaphore()

    @pl.loop(1, total)
    def _(step):
        pl.semaphore_signal(
            barrier, inc=1, device_id=device(lax.rem(linear + step, total)), device_id_type=MESH
        )

    load_grads.wait()
    pl.semaphore_wait(barrier, total - 1)

    def block(task, index):
        start, size = blocks[index]
        return every.at[task, :, pl.ds(start, size)]

    def send(index, target, slot, recv):
        return pltpu.make_async_remote_copy(
            src_ref=block(me, index),
            dst_ref=block(me, index),
            send_sem=send_sem.at[slot, index],
            recv_sem=recv,
            device_id={"task": target},
            device_id_type=MESH,
        )

    across = pltpu.make_async_remote_copy(
        src_ref=every.at[me],
        dst_ref=every.at[me],
        send_sem=send_sem.at[0, 0],
        recv_sem=near_recv.at[me],
        device_id={"task": partner},
        device_id_type=MESH,
    )
    across.start()

    for hop in range(1, chips):
        for index in live:
            other = lax.rem(chip + hop, chips)
            target = other * 2 + index % 2
            first = other == index // 2

            @pl.when(first)
            def _():
                send(index, target, hop, near_recv.at[me]).start()

    for hop in range(1, chips):
        for index in live:
            other = lax.rem(chip + hop, chips)
            target = other * 2 + index % 2
            first = other == index // 2

            @pl.when(jnp.logical_not(first))
            def _():
                send(index, target, hop, far_recv.at[me, index]).start()

    def forward(task, index):
        return pltpu.make_async_remote_copy(
            src_ref=block(task, index),
            dst_ref=block(task, index),
            send_sem=fwd_send.at[task, index],
            recv_sem=fwd_recv.at[task, index],
            device_id={"task": partner},
            device_id_type=MESH,
        )

    def waiter(ref, sem):
        return pltpu.make_async_copy(ref, ref, sem)

    load_acts.wait()
    acts = acts_v[...]
    outer = lax.dot_general(acts, acts, (((1,), (1,)), ((), ())), preferred_element_type=jnp.float32)
    high = outer.astype(jnp.bfloat16)
    rest = outer - high.astype(jnp.float32)
    mid = rest.astype(jnp.bfloat16)
    low = (rest - mid.astype(jnp.float32)).astype(jnp.bfloat16)
    kernel_mat[0:tokens] = high
    kernel_mat[tokens : 2 * tokens] = mid
    kernel_mat[2 * tokens :] = low

    def weigh(part):
        wide = jnp.dot(kernel_mat[...], part, preferred_element_type=jnp.float32)
        return wide[:tokens] + (wide[tokens : 2 * tokens] + wide[2 * tokens :])

    def fold(product):
        while product.shape[1] > LANES:
            half = product.shape[1] // 2
            product = product[:, :half] + product[:, half:]
        return jnp.sum(product.reshape(tokens // 8, 8, LANES), axis=0)

    rows_ref[...] = jnp.zeros_like(rows_ref)
    width = 2 * LANES if columns % (2 * LANES) == 0 else LANES
    for start in range(0, columns, width):
        part = every[me, :, start : start + width]
        prod = weigh(part)
        own_prod[:, start : start + width] = prod
        rows_ref[0] += fold(prod * part.astype(jnp.float32))
    waiter(every.at[partner], near_recv.at[partner]).wait()
    for start in range(0, columns, width):
        part = every[partner, :, start : start + width].astype(jnp.float32)
        rows_ref[1] += fold(own_prod[:, start : start + width] * part)

    tiles = columns // LANES
    first_tile = (tiles * me) // groups
    count = (tiles * (me + 1)) // groups - first_tile
    sizes = [size // LANES for _, size in blocks]

    def at(slot):
        return pl.ds(pl.multiple_of((first_tile + slot) * LANES, LANES), LANES)

    def over_share(body):
        for slot in range(max(sizes)):
            if slot < min(sizes):
                body(slot)
            else:
                pl.when(count > slot)(functools.partial(body, slot))

    def weigh_partner(slot):
        partner_prod[slot] = weigh(every[partner, :, at(slot)])

    over_share(weigh_partner)

    distant = []
    for hop in range(1, chips):
        for source_core in range(2):
            task = lax.rem(chip + hop, chips) * 2 + source_core
            distant.append((hop, task))
            for index in live:

                @pl.when(me == index)
                def _():
                    waiter(block(task, index), near_recv.at[task]).wait()
                    forward(task, index).start()

    pairs = [(me, me), (me, partner)]
    for _, task in distant:
        pairs += [(me, task), (partner, task)]
    for n, (hop, task) in enumerate(distant):
        pairs += [(task, late) for later, late in distant[n + 1 :] if later != hop]

    def cross(slot):
        parts = [every[task, :, at(slot)] for _, task in distant]
        wide = [part.astype(jnp.float32) for part in parts]
        own, near = own_prod[:, at(slot)], partner_prod[slot]
        spot = 2
        for part in wide:
            rows_ref[spot] += fold(own * part)
            rows_ref[spot + 1] += fold(near * part)
            spot += 2
        for n, (hop, _) in enumerate(distant):
            if any(later != hop for later, _ in distant[n + 1 :]):
                prod = weigh(parts[n])
                for k in range(n + 1, len(distant)):
                    if distant[k][0] != hop:
                        rows_ref[spot] += fold(prod * wide[k])
                        spot += 1

    over_share(cross)
    sums = jnp.sum(jnp.sum(rows_ref[...], axis=1), axis=1, keepdims=True)
    lane = lax.broadcasted_iota(jnp.int32, (1, LANES), 1)
    row = jnp.zeros((1, LANES), jnp.float32)
    for spot, (i, j) in enumerate(pairs):
        entry = sums[spot : spot + 1]
        if spot == 1:
            entry = 0.5 * entry
        row += jnp.where((lane == i * groups + j) | (lane == j * groups + i), entry, 0.0)
    mine_ref[...] = row
    gath[linear] = row

    @pl.loop(1, total)
    def _(step):
        pltpu.make_async_remote_copy(
            src_ref=mine_ref,
            dst_ref=gath.at[linear],
            send_sem=row_send,
            recv_sem=row_recv,
            device_id=device(lax.rem(linear + step, total)),
            device_id_type=MESH,
        ).start()

    for hop in range(1, chips):
        other = lax.rem(chip + hop, chips)
        for index in live:
            for source_core in range(2):
                task = other * 2 + source_core

                @pl.when((chip != index // 2) & (core == index % 2))
                def _():
                    waiter(block(task, index), far_recv.at[task, index]).wait()
                    forward(task, index).start()

    for hop in range(1, chips):
        other = lax.rem(chip + hop, chips)
        for index in live:
            for source_core in range(2):
                task = other * 2 + source_core

                @pl.when(core != index % 2)
                def _():
                    waiter(block(task, index), fwd_recv.at[task, index]).wait()

    part_rows = acts_t.shape[0]
    if part_rows % LANES == 0:
        for start in range(0, part_rows, LANES):
            source = pl.ds(pl.multiple_of(me * part_rows + start, LANES), LANES)
            acts_t[start : start + LANES, :] = acts_v[:, source].T
    else:
        for start in range(0, acts_v.shape[1], LANES):
            turned[start : start + LANES, :] = acts_v[:, start : start + LANES].T
        acts_t[...] = turned[pl.ds(pl.multiple_of(me * part_rows, 16), part_rows), :]

    bulk = gath.at[pl.ds(0, total - 1)]
    waiter(bulk, row_recv).wait()
    gram_row = jnp.sum(gath[...], axis=0)
    weights = pcgrad_weights(gram_row, order_ref, groups)

    @pl.loop(0, tiles)
    def _(tile):
        at = pl.ds(pl.multiple_of(tile * LANES, LANES), LANES)
        mixed = weights[0:1] * every[0, :, at].astype(jnp.float32)
        for k in range(1, groups):
            mixed = mixed + weights[k : k + 1] * every[k, :, at].astype(jnp.float32)
        combined_ref[:, at] = mixed.astype(jnp.bfloat16)

    diagonal = lax.broadcasted_iota(jnp.int32, (weights.shape[0], LANES), 0) == (
        lax.broadcasted_iota(jnp.int32, (weights.shape[0], LANES), 1)
    )
    weights_ref[...] = jnp.sum(jnp.where(diagonal, weights, 0.0), axis=0, keepdims=True)

    waiter(bulk, row_send).wait()
    waiter(every.at[me], send_sem.at[0, 0]).wait()
    for hop in range(1, chips):
        other = lax.rem(chip + hop, chips)
        for index in live:
            waiter(block(me, index), send_sem.at[hop, index]).wait()
            for source_core in range(2):
                task = other * 2 + source_core

                @pl.when(core == index % 2)
                def _():
                    waiter(block(task, index), fwd_send.at[task, index]).wait()


def expand(acts_t, combined, weights_row, update_hbm, weights_ref, buffer, sems):
    rows = acts_t.shape[0]
    step = LANES if rows % LANES == 0 else rows
    copies = []
    for n, start in enumerate(range(0, rows, step)):
        span = pl.ds(start, step)
        buffer[span, :] = jnp.dot(
            acts_t[span, :], combined[...], preferred_element_type=jnp.float32
        )
        copy = pltpu.make_async_copy(buffer.at[span], update_hbm.at[span], sems.at[n])
        copy.start()
        copies.append(copy)
    weights_ref[...] = weights_row[0, : weights_ref.shape[0]]
    for copy in copies:
        copy.wait()


def shards(acts, out_grads, order):
    groups = lax.axis_size("task")
    others = lax.axis_size("param")
    total = groups * others
    tokens, columns = out_grads.shape[1:]
    model = acts.shape[1]
    part_rows = model // groups
    most = max(size for _, size in column_blocks(columns, groups)) // LANES
    remote = groups - 2
    pair_count = 2 + 2 * remote + remote * (remote - 2) // 2
    aligned = part_rows % LANES == 0
    kept = 2 * tokens * (columns + part_rows) + 2**16
    dma = pltpu.SemaphoreType.DMA
    vmem = pl.BlockSpec(memory_space=pltpu.VMEM)
    combined, acts_t, weights_row = pl.pallas_call(
        functools.partial(mixer, groups, others),
        out_shape=(
            pltpu.VMEM((tokens, columns), jnp.bfloat16),
            pltpu.VMEM((part_rows, tokens), jnp.bfloat16),
            pltpu.VMEM((1, LANES), jnp.float32),
        ),
        in_specs=[
            pl.BlockSpec(memory_space=pltpu.SMEM),
            pl.BlockSpec(memory_space=pltpu.HBM),
            pl.BlockSpec(memory_space=pltpu.HBM),
        ],
        out_specs=(vmem, vmem, vmem),
        scratch_shapes=[
            pltpu.VMEM(acts.shape, jnp.bfloat16),
            pltpu.VMEM((groups, tokens, columns), jnp.bfloat16),
            pltpu.VMEM((3 * tokens, tokens), jnp.bfloat16),
            pltpu.VMEM((tokens, columns), jnp.float32),
            pltpu.VMEM((most, tokens, LANES), jnp.float32),
            pltpu.VMEM((pair_count, 8, LANES), jnp.float32),
            pltpu.VMEM((16 if aligned else model, tokens), jnp.bfloat16),
            pltpu.VMEM((1, LANES), jnp.float32),
            pltpu.VMEM((total, 1, LANES), jnp.float32),
            dma((2,)),
            dma((groups, groups)),
            dma((groups,)),
            dma((groups, groups)),
            dma((groups, groups)),
            dma((groups, groups)),
            dma,
            dma,
        ],
        compiler_params=pltpu.CompilerParams(
            collective_id=0, has_side_effects=True, vmem_limit_bytes=VMEM_BYTES - kept
        ),
        name="mixer",
    )(order, acts, out_grads)
    update, weights = pl.pallas_call(
        expand,
        out_shape=(
            jax.ShapeDtypeStruct((part_rows, columns), jnp.float32),
            jax.ShapeDtypeStruct((groups,), jnp.float32),
        ),
        in_specs=[vmem, vmem, vmem],
        out_specs=(pl.BlockSpec(memory_space=pl.ANY), vmem),
        scratch_shapes=[
            pltpu.VMEM((part_rows, columns), jnp.float32),
            dma((pl.cdiv(part_rows, LANES),)),
        ],
        compiler_params=pltpu.CompilerParams(vmem_limit_bytes=24 * 2**20),
        name="expand",
    )(acts_t, combined, weights_row)
    return (update, weights)


def solution(mesh):
    in_specs = (P(), P("task", None, "param"), P())
    out_specs = (P("task", "param"), P())
    return jax.shard_map(shards, mesh=mesh, in_specs=in_specs, out_specs=out_specs, check_vma=False)
```

```python
import functools

import jax
import jax.numpy as jnp
from jax import lax
from jax.experimental import pallas as pl
from jax.experimental.pallas import tpu as pltpu
from jax.sharding import PartitionSpec as P

MESH = pl.DeviceIdType.MESH
LANES = 128
VMEM_BYTES = 67043328


def column_blocks(columns, groups):
    tiles = columns // LANES
    edges = [tiles * g // groups for g in range(groups + 1)]
    return [(edges[g] * LANES, (edges[g + 1] - edges[g]) * LANES) for g in range(groups)]


def pcgrad_weights(gram_row, order_ref, tasks):
    rows = max(8, tasks)
    sub = lax.broadcasted_iota(jnp.int32, (rows, LANES), 0)
    lane = lax.broadcasted_iota(jnp.int32, (rows, LANES), 1)
    flat = jnp.broadcast_to(gram_row, (rows, LANES))
    targets, columns, scales = [], [], []
    for step in range(tasks):
        target = order_ref[step]
        column = jnp.sum(jnp.where(lane == sub * tasks + target, flat, 0.0), axis=1, keepdims=True)
        scale = jnp.sum(jnp.where(lane == target * (tasks + 1), flat, 0.0), axis=1, keepdims=True)
        targets.append(target)
        columns.append(jnp.broadcast_to(column, (rows, LANES)))
        scales.append(scale[:1] + 1e-6)
    mix = jnp.where((sub == lane) & (sub < tasks), 1.0, 0.0)
    for target, column, scale in zip(targets, columns, scales):
        dots = jnp.sum(mix * column, axis=0, keepdims=True)
        change = jnp.minimum(dots, 0.0) / scale
        mix = mix - jnp.where((sub == target) & (lane != target), change, 0.0)
    return jnp.sum(mix, axis=1, keepdims=True)


def mixer(
    groups,
    others,
    order_ref,
    acts_hbm,
    grads_hbm,
    combined_ref,
    acts_t,
    weights_ref,
    acts_v,
    every,
    kernel_mat,
    own_prod,
    partner_prod,
    rows_ref,
    turned,
    mine_ref,
    gath,
    local_sem,
    send_sem,
    near_recv,
    far_recv,
    fwd_send,
    fwd_recv,
    row_send,
    row_recv,
    round_sem,
):
    me = lax.axis_index("task")
    place = lax.axis_index("param")
    core = lax.rem(me, 2)
    partner = me + 1 - 2 * core
    total = groups * others
    chips = groups // 2
    chip = me // 2
    linear = me * others + place
    tokens, columns = every.shape[1:]
    blocks = column_blocks(columns, groups)
    live = [index for index in range(groups) if blocks[index][1] > 0]

    load_grads = pltpu.make_async_copy(grads_hbm.at[0], every.at[me], local_sem.at[0])
    load_acts = pltpu.make_async_copy(acts_hbm, acts_v, local_sem.at[1])
    load_grads.start()
    load_acts.start()

    bits = (others - 1).bit_length()
    doubling = others == 1 << bits

    def flipped(mask):
        index = place
        for bit in range(bits):
            if mask >> bit & 1:
                index = index + (1 << bit) * (1 - 2 * lax.rem(place // (1 << bit), 2))
        return index

    def signal(semaphore, device):
        pl.semaphore_signal(semaphore, inc=1, device_id=device, device_id_type=MESH)

    tasks_from_me = [lax.rem(me + step, groups) for step in range(groups)]
    if doubling:
        places_from_me = [flipped(mask) for mask in range(others)]
    else:
        places_from_me = [lax.rem(place + step, others) for step in range(others)]
    peers = [
        {"task": task, "param": spot}
        for far, spot in reversed(list(enumerate(places_from_me)))
        for step, task in reversed(list(enumerate(tasks_from_me)))
        if far or step
    ]

    barrier = pltpu.get_barrier_semaphore()
    if doubling:
        greeted = [{"task": task} for task in tasks_from_me[1:]]
        greeted += [{"param": flipped(1 << bit)} for bit in range(bits)]
    else:
        greeted = peers
    for device in greeted:
        signal(barrier, device)
    load_grads.wait()
    pl.semaphore_wait(barrier, len(greeted))

    def block(task, index):
        start, size = blocks[index]
        return every.at[task, :, pl.ds(start, size)]

    def send(index, target, slot, recv):
        return pltpu.make_async_remote_copy(
            src_ref=block(me, index),
            dst_ref=block(me, index),
            send_sem=send_sem.at[slot, index],
            recv_sem=recv,
            device_id={"task": target},
            device_id_type=MESH,
        )

    across = pltpu.make_async_remote_copy(
        src_ref=every.at[me],
        dst_ref=every.at[me],
        send_sem=send_sem.at[0, 0],
        recv_sem=near_recv.at[me],
        device_id={"task": partner},
        device_id_type=MESH,
    )
    across.start()

    for hop in range(1, chips):
        for index in live:
            other = lax.rem(chip + hop, chips)
            target = other * 2 + index % 2
            first = other == index // 2

            @pl.when(first)
            def _():
                send(index, target, hop, near_recv.at[me]).start()

    for hop in range(1, chips):
        for index in live:
            other = lax.rem(chip + hop, chips)
            target = other * 2 + index % 2
            first = other == index // 2

            @pl.when(jnp.logical_not(first))
            def _():
                send(index, target, hop, far_recv.at[me, index]).start()

    def forward(task, index):
        return pltpu.make_async_remote_copy(
            src_ref=block(task, index),
            dst_ref=block(task, index),
            send_sem=fwd_send.at[task, index],
            recv_sem=fwd_recv.at[task, index],
            device_id={"task": partner},
            device_id_type=MESH,
        )

    def waiter(ref, sem):
        return pltpu.make_async_copy(ref, ref, sem)

    def spread(bit):
        if doubling and bit < bits:
            signal(round_sem.at[bit], {"param": flipped(1 << bit)})

    def learn(bit):
        if doubling and bit < bits:
            pl.semaphore_wait(round_sem.at[bit], 1)

    spread(0)
    load_acts.wait()
    acts = acts_v[...]
    outer = lax.dot_general(acts, acts, (((1,), (1,)), ((), ())), preferred_element_type=jnp.float32)
    high = outer.astype(jnp.bfloat16)
    rest = outer - high.astype(jnp.float32)
    mid = rest.astype(jnp.bfloat16)
    low = (rest - mid.astype(jnp.float32)).astype(jnp.bfloat16)
    kernel_mat[0:tokens] = high
    kernel_mat[tokens : 2 * tokens] = mid
    kernel_mat[2 * tokens :] = low

    def weigh(part):
        wide = jnp.dot(kernel_mat[...], part, preferred_element_type=jnp.float32)
        return wide[:tokens] + (wide[tokens : 2 * tokens] + wide[2 * tokens :])

    def fold(product):
        while product.shape[1] > LANES:
            half = product.shape[1] // 2
            product = product[:, :half] + product[:, half:]
        return jnp.sum(product.reshape(tokens // 8, 8, LANES), axis=0)

    rows_ref[...] = jnp.zeros_like(rows_ref)
    width = 2 * LANES if columns % (2 * LANES) == 0 else LANES
    for start in range(0, columns, width):
        part = every[me, :, start : start + width]
        prod = weigh(part)
        own_prod[:, start : start + width] = prod
        rows_ref[0] += fold(prod * part.astype(jnp.float32))
    waiter(every.at[partner], near_recv.at[partner]).wait()
    for start in range(0, columns, width):
        part = every[partner, :, start : start + width].astype(jnp.float32)
        rows_ref[1] += fold(own_prod[:, start : start + width] * part)

    tiles = columns // LANES
    first_tile = (tiles * me) // groups
    count = (tiles * (me + 1)) // groups - first_tile
    sizes = [size // LANES for _, size in blocks]

    def at(slot):
        return pl.ds(pl.multiple_of((first_tile + slot) * LANES, LANES), LANES)

    def over_share(body):
        for slot in range(max(sizes)):
            if slot < min(sizes):
                body(slot)
            else:
                pl.when(count > slot)(functools.partial(body, slot))

    def weigh_partner(slot):
        partner_prod[slot] = weigh(every[partner, :, at(slot)])

    over_share(weigh_partner)
    for bit in range(bits):
        if bit > 0:
            spread(bit)
        learn(bit)

    distant = []
    for hop in range(1, chips):
        for source_core in range(2):
            task = lax.rem(chip + hop, chips) * 2 + source_core
            distant.append((hop, task))
            for index in live:

                @pl.when(me == index)
                def _():
                    waiter(block(task, index), near_recv.at[task]).wait()
                    forward(task, index).start()

    pairs = [(me, me), (me, partner)]
    for _, task in distant:
        pairs += [(me, task), (partner, task)]
    for n, (hop, task) in enumerate(distant):
        pairs += [(task, late) for later, late in distant[n + 1 :] if later != hop]

    def cross(slot):
        parts = [every[task, :, at(slot)] for _, task in distant]
        wide = [part.astype(jnp.float32) for part in parts]
        own, near = own_prod[:, at(slot)], partner_prod[slot]
        spot = 2
        for part in wide:
            rows_ref[spot] += fold(own * part)
            rows_ref[spot + 1] += fold(near * part)
            spot += 2
        for n, (hop, _) in enumerate(distant):
            if any(later != hop for later, _ in distant[n + 1 :]):
                prod = weigh(parts[n])
                for k in range(n + 1, len(distant)):
                    if distant[k][0] != hop:
                        rows_ref[spot] += fold(prod * wide[k])
                        spot += 1

    over_share(cross)
    sums = jnp.sum(jnp.sum(rows_ref[...], axis=1), axis=1, keepdims=True)
    lane = lax.broadcasted_iota(jnp.int32, (1, LANES), 1)
    row = jnp.zeros((1, LANES), jnp.float32)
    for spot, (i, j) in enumerate(pairs):
        entry = sums[spot : spot + 1]
        if spot == 1:
            entry = 0.5 * entry
        row += jnp.where((lane == i * groups + j) | (lane == j * groups + i), entry, 0.0)
    mine_ref[...] = row
    gath[linear] = row

    for device in peers:
        pltpu.make_async_remote_copy(
            src_ref=mine_ref,
            dst_ref=gath.at[linear],
            send_sem=row_send,
            recv_sem=row_recv,
            device_id=device,
            device_id_type=MESH,
        ).start()

    for hop in range(1, chips):
        other = lax.rem(chip + hop, chips)
        for index in live:
            for source_core in range(2):
                task = other * 2 + source_core

                @pl.when((chip != index // 2) & (core == index % 2))
                def _():
                    waiter(block(task, index), far_recv.at[task, index]).wait()
                    forward(task, index).start()

    for hop in range(1, chips):
        other = lax.rem(chip + hop, chips)
        for index in live:
            for source_core in range(2):
                task = other * 2 + source_core

                @pl.when(core != index % 2)
                def _():
                    waiter(block(task, index), fwd_recv.at[task, index]).wait()

    part_rows = acts_t.shape[0]
    if part_rows % LANES == 0:
        for start in range(0, part_rows, LANES):
            source = pl.ds(pl.multiple_of(me * part_rows + start, LANES), LANES)
            acts_t[start : start + LANES, :] = acts_v[:, source].T
    else:
        for start in range(0, acts_v.shape[1], LANES):
            turned[start : start + LANES, :] = acts_v[:, start : start + LANES].T
        acts_t[...] = turned[pl.ds(pl.multiple_of(me * part_rows, 16), part_rows), :]

    bulk = gath.at[pl.ds(0, total - 1)]
    waiter(bulk, row_recv).wait()
    gram_row = jnp.sum(gath[...], axis=0)
    weights = pcgrad_weights(gram_row, order_ref, groups)

    @pl.loop(0, tiles)
    def _(tile):
        at = pl.ds(pl.multiple_of(tile * LANES, LANES), LANES)
        mixed = weights[0:1] * every[0, :, at].astype(jnp.float32)
        for k in range(1, groups):
            mixed = mixed + weights[k : k + 1] * every[k, :, at].astype(jnp.float32)
        combined_ref[:, at] = mixed.astype(jnp.bfloat16)

    diagonal = lax.broadcasted_iota(jnp.int32, (weights.shape[0], LANES), 0) == (
        lax.broadcasted_iota(jnp.int32, (weights.shape[0], LANES), 1)
    )
    weights_ref[...] = jnp.sum(jnp.where(diagonal, weights, 0.0), axis=0, keepdims=True)

    waiter(bulk, row_send).wait()
    waiter(every.at[me], send_sem.at[0, 0]).wait()
    for hop in range(1, chips):
        other = lax.rem(chip + hop, chips)
        for index in live:
            waiter(block(me, index), send_sem.at[hop, index]).wait()
            for source_core in range(2):
                task = other * 2 + source_core

                @pl.when(core == index % 2)
                def _():
                    waiter(block(task, index), fwd_send.at[task, index]).wait()


def expand(acts_t, combined, weights_row, update_hbm, weights_ref, buffer, sems):
    rows = acts_t.shape[0]
    step = LANES if rows % LANES == 0 else rows
    copies = []
    for n, start in enumerate(range(0, rows, step)):
        span = pl.ds(start, step)
        buffer[span, :] = jnp.dot(
            acts_t[span, :], combined[...], preferred_element_type=jnp.float32
        )
        copy = pltpu.make_async_copy(buffer.at[span], update_hbm.at[span], sems.at[n])
        copy.start()
        copies.append(copy)
    weights_ref[...] = weights_row[0, : weights_ref.shape[0]]
    for copy in copies:
        copy.wait()


def shards(acts, out_grads, order):
    groups = lax.axis_size("task")
    others = lax.axis_size("param")
    total = groups * others
    tokens, columns = out_grads.shape[1:]
    model = acts.shape[1]
    part_rows = model // groups
    most = max(size for _, size in column_blocks(columns, groups)) // LANES
    remote = groups - 2
    pair_count = 2 + 2 * remote + remote * (remote - 2) // 2
    aligned = part_rows % LANES == 0
    kept = 2 * tokens * (columns + part_rows) + 2**16
    dma = pltpu.SemaphoreType.DMA
    vmem = pl.BlockSpec(memory_space=pltpu.VMEM)
    combined, acts_t, weights_row = pl.pallas_call(
        functools.partial(mixer, groups, others),
        out_shape=(
            pltpu.VMEM((tokens, columns), jnp.bfloat16),
            pltpu.VMEM((part_rows, tokens), jnp.bfloat16),
            pltpu.VMEM((1, LANES), jnp.float32),
        ),
        in_specs=[
            pl.BlockSpec(memory_space=pltpu.SMEM),
            pl.BlockSpec(memory_space=pltpu.HBM),
            pl.BlockSpec(memory_space=pltpu.HBM),
        ],
        out_specs=(vmem, vmem, vmem),
        scratch_shapes=[
            pltpu.VMEM(acts.shape, jnp.bfloat16),
            pltpu.VMEM((groups, tokens, columns), jnp.bfloat16),
            pltpu.VMEM((3 * tokens, tokens), jnp.bfloat16),
            pltpu.VMEM((tokens, columns), jnp.float32),
            pltpu.VMEM((most, tokens, LANES), jnp.float32),
            pltpu.VMEM((pair_count, 8, LANES), jnp.float32),
            pltpu.VMEM((16 if aligned else model, tokens), jnp.bfloat16),
            pltpu.VMEM((1, LANES), jnp.float32),
            pltpu.VMEM((total, 1, LANES), jnp.float32),
            dma((2,)),
            dma((groups, groups)),
            dma((groups,)),
            dma((groups, groups)),
            dma((groups, groups)),
            dma((groups, groups)),
            dma,
            dma,
            pltpu.SemaphoreType.REGULAR((max(1, (others - 1).bit_length()),)),
        ],
        compiler_params=pltpu.CompilerParams(
            collective_id=0, has_side_effects=True, vmem_limit_bytes=VMEM_BYTES - kept
        ),
        name="mixer",
    )(order, acts, out_grads)
    update, weights = pl.pallas_call(
        expand,
        out_shape=(
            jax.ShapeDtypeStruct((part_rows, columns), jnp.float32),
            jax.ShapeDtypeStruct((groups,), jnp.float32),
        ),
        in_specs=[vmem, vmem, vmem],
        out_specs=(pl.BlockSpec(memory_space=pl.ANY), vmem),
        scratch_shapes=[
            pltpu.VMEM((part_rows, columns), jnp.float32),
            dma((pl.cdiv(part_rows, LANES),)),
        ],
        compiler_params=pltpu.CompilerParams(vmem_limit_bytes=24 * 2**20),
        name="expand",
    )(acts_t, combined, weights_row)
    return (update, weights)


def solution(mesh):
    in_specs = (P(), P("task", None, "param"), P())
    out_specs = (P("task", "param"), P())
    return jax.shard_map(shards, mesh=mesh, in_specs=in_specs, out_specs=out_specs, check_vma=False)
```

```python
import functools

import jax
import jax.numpy as jnp
from jax import lax
from jax.experimental import pallas as pl
from jax.experimental.pallas import tpu as pltpu
from jax.sharding import PartitionSpec as P

MESH = pl.DeviceIdType.MESH
LANES = 128
VMEM_BYTES = 67043328


def column_blocks(columns, groups):
    tiles = columns // LANES
    edges = [tiles * g // groups for g in range(groups + 1)]
    return [(edges[g] * LANES, (edges[g + 1] - edges[g]) * LANES) for g in range(groups)]


def pcgrad_weights(gram_row, order_ref, tasks):
    rows = max(8, tasks)
    sub = lax.broadcasted_iota(jnp.int32, (rows, LANES), 0)
    lane = lax.broadcasted_iota(jnp.int32, (rows, LANES), 1)
    flat = jnp.broadcast_to(gram_row, (rows, LANES))
    targets, columns, scales = [], [], []
    for step in range(tasks):
        target = order_ref[step]
        column = jnp.sum(jnp.where(lane == sub * tasks + target, flat, 0.0), axis=1, keepdims=True)
        scale = jnp.sum(jnp.where(lane == target * (tasks + 1), flat, 0.0), axis=1, keepdims=True)
        targets.append(target)
        columns.append(jnp.broadcast_to(column, (rows, LANES)))
        scales.append(1.0 / (scale[:1] + 1e-6))
    mix = jnp.where((sub == lane) & (sub < tasks), 1.0, 0.0)
    for target, column, scale in zip(targets, columns, scales):
        dots = jnp.sum(mix * column, axis=0, keepdims=True)
        change = jnp.minimum(dots, 0.0) * scale
        mix = mix - jnp.where((sub == target) & (lane != target), change, 0.0)
    return jnp.sum(mix, axis=1, keepdims=True)


def mixer(
    groups,
    others,
    order_hbm,
    acts_hbm,
    grads_hbm,
    combined_ref,
    acts_t,
    weights_ref,
    acts_v,
    every,
    kernel_mat,
    own_prod,
    partner_prod,
    rows_ref,
    turned,
    mine_ref,
    gath,
    local_sem,
    send_sem,
    near_recv,
    far_recv,
    fwd_send,
    fwd_recv,
    row_send,
    row_recv,
    round_sem,
    order_ref,
):
    me = lax.axis_index("task")
    place = lax.axis_index("param")
    core = lax.rem(me, 2)
    partner = me + 1 - 2 * core
    total = groups * others
    chips = groups // 2
    chip = me // 2
    linear = me * others + place
    tokens, columns = every.shape[1:]
    blocks = column_blocks(columns, groups)
    live = [index for index in range(groups) if blocks[index][1] > 0]

    load_grads = pltpu.make_async_copy(grads_hbm.at[0], every.at[me], local_sem.at[0])
    load_acts = pltpu.make_async_copy(acts_hbm, acts_v, local_sem.at[1])
    load_grads.start()
    load_acts.start()
    load_order = pltpu.make_async_copy(order_hbm, order_ref, local_sem.at[2])
    load_order.start()

    bits = (others - 1).bit_length()
    doubling = others == 1 << bits

    def flipped(mask):
        index = place
        for bit in range(bits):
            if mask >> bit & 1:
                index = index + (1 << bit) * (1 - 2 * lax.rem(place // (1 << bit), 2))
        return index

    def signal(semaphore, device):
        pl.semaphore_signal(semaphore, inc=1, device_id=device, device_id_type=MESH)

    tasks_from_me = [lax.rem(me + step, groups) for step in range(groups)]
    if doubling:
        places_from_me = [flipped(mask) for mask in range(others)]
    else:
        places_from_me = [lax.rem(place + step, others) for step in range(others)]
    peers = [
        {"task": task, "param": spot}
        for far, spot in reversed(list(enumerate(places_from_me)))
        for step, task in reversed(list(enumerate(tasks_from_me)))
        if far or step
    ]

    barrier = pltpu.get_barrier_semaphore()
    if doubling:
        greeted = [{"task": task} for task in tasks_from_me[1:]]
        greeted += [{"param": flipped(1 << bit)} for bit in range(bits)]
    else:
        greeted = peers
    for device in greeted:
        signal(barrier, device)
    load_grads.wait()
    pl.semaphore_wait(barrier, len(greeted))

    def block(task, index):
        start, size = blocks[index]
        return every.at[task, :, pl.ds(start, size)]

    def send(index, target, slot, recv):
        return pltpu.make_async_remote_copy(
            src_ref=block(me, index),
            dst_ref=block(me, index),
            send_sem=send_sem.at[slot, index],
            recv_sem=recv,
            device_id={"task": target},
            device_id_type=MESH,
        )

    across = pltpu.make_async_remote_copy(
        src_ref=every.at[me],
        dst_ref=every.at[me],
        send_sem=send_sem.at[0, 0],
        recv_sem=near_recv.at[me],
        device_id={"task": partner},
        device_id_type=MESH,
    )
    across.start()

    for hop in range(1, chips):
        for index in live:
            other = lax.rem(chip + hop, chips)
            target = other * 2 + index % 2
            first = other == index // 2

            @pl.when(first)
            def _():
                send(index, target, hop, near_recv.at[me]).start()

    def send_rest(parity):
        for hop in range(1, chips):
            for index in live:
                if index % 2 == parity:
                    other = lax.rem(chip + hop, chips)
                    target = other * 2 + index % 2

                    @pl.when(other != index // 2)
                    def _():
                        send(index, target, hop, far_recv.at[me, index]).start()

    send_rest(1)

    def forward(task, index):
        return pltpu.make_async_remote_copy(
            src_ref=block(task, index),
            dst_ref=block(task, index),
            send_sem=fwd_send.at[task, index],
            recv_sem=fwd_recv.at[task, index],
            device_id={"task": partner},
            device_id_type=MESH,
        )

    def waiter(ref, sem):
        return pltpu.make_async_copy(ref, ref, sem)

    def spread(bit):
        if doubling and bit < bits:
            signal(round_sem.at[bit], {"param": flipped(1 << bit)})

    def learn(bit):
        if doubling and bit < bits:
            pl.semaphore_wait(round_sem.at[bit], 1)

    spread(0)
    load_acts.wait()
    acts = acts_v[...]
    outer = lax.dot_general(acts, acts, (((1,), (1,)), ((), ())), preferred_element_type=jnp.float32)
    high = outer.astype(jnp.bfloat16)
    rest = outer - high.astype(jnp.float32)
    mid = rest.astype(jnp.bfloat16)
    low = (rest - mid.astype(jnp.float32)).astype(jnp.bfloat16)
    kernel_mat[0:tokens] = high
    kernel_mat[tokens : 2 * tokens] = mid
    kernel_mat[2 * tokens :] = low

    def weigh(part):
        wide = jnp.dot(kernel_mat[...], part, preferred_element_type=jnp.float32)
        return wide[:tokens] + (wide[tokens : 2 * tokens] + wide[2 * tokens :])

    def fold(product):
        while product.shape[1] > LANES:
            half = product.shape[1] // 2
            product = product[:, :half] + product[:, half:]
        return jnp.sum(product.reshape(tokens // 8, 8, LANES), axis=0)

    rows_ref[...] = jnp.zeros_like(rows_ref)
    width = 2 * LANES if columns % (2 * LANES) == 0 else LANES
    for start in range(0, columns, width):
        part = every[me, :, start : start + width]
        prod = weigh(part)
        own_prod[:, start : start + width] = prod
        rows_ref[0] += fold(prod * part.astype(jnp.float32))
    waiter(every.at[partner], near_recv.at[partner]).wait()
    for start in range(0, columns, width):
        part = every[partner, :, start : start + width].astype(jnp.float32)
        rows_ref[1] += fold(own_prod[:, start : start + width] * part)

    tiles = columns // LANES
    first_tile = (tiles * me) // groups
    count = (tiles * (me + 1)) // groups - first_tile
    sizes = [size // LANES for _, size in blocks]

    def at(slot):
        return pl.ds(pl.multiple_of((first_tile + slot) * LANES, LANES), LANES)

    def over_share(body):
        for slot in range(max(sizes)):
            if slot < min(sizes):
                body(slot)
            else:
                pl.when(count > slot)(functools.partial(body, slot))

    def weigh_partner(slot):
        partner_prod[slot] = weigh(every[partner, :, at(slot)])

    over_share(weigh_partner)
    for bit in range(bits):
        if bit > 0:
            spread(bit)
        learn(bit)

    distant = []
    for hop in range(1, chips):
        for source_core in range(2):
            task = lax.rem(chip + hop, chips) * 2 + source_core
            distant.append((hop, task))
            for index in live:

                @pl.when(me == index)
                def _():
                    waiter(block(task, index), near_recv.at[task]).wait()
                    forward(task, index).start()

    pairs = [(me, me), (me, partner)]
    for _, task in distant:
        pairs += [(me, task), (partner, task)]
    for n, (hop, task) in enumerate(distant):
        pairs += [(task, late) for later, late in distant[n + 1 :] if later != hop]

    def cross(slot):
        parts = [every[task, :, at(slot)] for _, task in distant]
        wide = [part.astype(jnp.float32) for part in parts]
        own, near = own_prod[:, at(slot)], partner_prod[slot]
        spot = 2
        for part in wide:
            rows_ref[spot] += fold(own * part)
            rows_ref[spot + 1] += fold(near * part)
            spot += 2
        for n, (hop, _) in enumerate(distant):
            if any(later != hop for later, _ in distant[n + 1 :]):
                prod = weigh(parts[n])
                for k in range(n + 1, len(distant)):
                    if distant[k][0] != hop:
                        rows_ref[spot] += fold(prod * wide[k])
                        spot += 1

    over_share(cross)
    sums = jnp.sum(jnp.sum(rows_ref[...], axis=1), axis=1, keepdims=True)
    lane = lax.broadcasted_iota(jnp.int32, (1, LANES), 1)
    row = jnp.zeros((1, LANES), jnp.float32)
    for spot, (i, j) in enumerate(pairs):
        entry = sums[spot : spot + 1]
        if spot == 1:
            entry = 0.5 * entry
        row += jnp.where((lane == i * groups + j) | (lane == j * groups + i), entry, 0.0)
    mine_ref[...] = row
    gath[linear] = row

    for device in peers:
        pltpu.make_async_remote_copy(
            src_ref=mine_ref,
            dst_ref=gath.at[linear],
            send_sem=row_send,
            recv_sem=row_recv,
            device_id=device,
            device_id_type=MESH,
        ).start()

    send_rest(0)

    for hop in range(1, chips):
        other = lax.rem(chip + hop, chips)
        for index in live:
            for source_core in range(2):
                task = other * 2 + source_core

                @pl.when((chip != index // 2) & (core == index % 2))
                def _():
                    waiter(block(task, index), far_recv.at[task, index]).wait()
                    forward(task, index).start()

    for hop in range(1, chips):
        other = lax.rem(chip + hop, chips)
        for index in live:
            for source_core in range(2):
                task = other * 2 + source_core

                @pl.when(core != index % 2)
                def _():
                    waiter(block(task, index), fwd_recv.at[task, index]).wait()

    part_rows = acts_t.shape[0]
    if part_rows % LANES == 0:
        for start in range(0, part_rows, LANES):
            source = pl.ds(pl.multiple_of(me * part_rows + start, LANES), LANES)
            acts_t[start : start + LANES, :] = acts_v[:, source].T
    else:
        for start in range(0, acts_v.shape[1], LANES):
            turned[start : start + LANES, :] = acts_v[:, start : start + LANES].T
        acts_t[...] = turned[pl.ds(pl.multiple_of(me * part_rows, 16), part_rows), :]

    load_order.wait()
    bulk = gath.at[pl.ds(0, total - 1)]
    waiter(bulk, row_recv).wait()
    gram_row = jnp.sum(gath[...], axis=0)
    weights = pcgrad_weights(gram_row, order_ref, groups)

    @pl.loop(0, tiles, unroll=True)
    def _(tile):
        at = pl.ds(pl.multiple_of(tile * LANES, LANES), LANES)
        mixed = weights[0:1] * every[0, :, at].astype(jnp.float32)
        for k in range(1, groups):
            mixed = mixed + weights[k : k + 1] * every[k, :, at].astype(jnp.float32)
        combined_ref[:, at] = mixed.astype(jnp.bfloat16)

    diagonal = lax.broadcasted_iota(jnp.int32, (weights.shape[0], LANES), 0) == (
        lax.broadcasted_iota(jnp.int32, (weights.shape[0], LANES), 1)
    )
    weights_ref[...] = jnp.sum(jnp.where(diagonal, weights, 0.0), axis=0, keepdims=True)

    waiter(bulk, row_send).wait()
    waiter(every.at[me], send_sem.at[0, 0]).wait()
    for hop in range(1, chips):
        other = lax.rem(chip + hop, chips)
        for index in live:
            waiter(block(me, index), send_sem.at[hop, index]).wait()
            for source_core in range(2):
                task = other * 2 + source_core

                @pl.when(core == index % 2)
                def _():
                    waiter(block(task, index), fwd_send.at[task, index]).wait()


def expand(acts_t, combined, weights_row, update_hbm, weights_hbm, buffer, few, sems, few_sem):
    few[...] = weights_row[0, : few.shape[0]]
    small = pltpu.make_async_copy(few, weights_hbm, few_sem)
    small.start()
    rows = acts_t.shape[0]
    step = LANES if rows % LANES == 0 else rows
    copies = []
    for n, start in enumerate(range(0, rows, step)):
        span = pl.ds(start, step)
        buffer[span, :] = jnp.dot(
            acts_t[span, :], combined[...], preferred_element_type=jnp.float32
        )
        copy = pltpu.make_async_copy(buffer.at[span], update_hbm.at[span], sems.at[n])
        copy.start()
        copies.append(copy)
    for copy in copies:
        copy.wait()
    small.wait()


def shards(acts, out_grads, order):
    groups = lax.axis_size("task")
    others = lax.axis_size("param")
    total = groups * others
    tokens, columns = out_grads.shape[1:]
    model = acts.shape[1]
    part_rows = model // groups
    most = max(size for _, size in column_blocks(columns, groups)) // LANES
    remote = groups - 2
    pair_count = 2 + 2 * remote + remote * (remote - 2) // 2
    aligned = part_rows % LANES == 0
    kept = 2 * tokens * (columns + part_rows) + 2**16
    dma = pltpu.SemaphoreType.DMA
    vmem = pl.BlockSpec(memory_space=pltpu.VMEM)
    combined, acts_t, weights_row = pl.pallas_call(
        functools.partial(mixer, groups, others),
        out_shape=(
            pltpu.VMEM((tokens, columns), jnp.bfloat16),
            pltpu.VMEM((part_rows, tokens), jnp.bfloat16),
            pltpu.VMEM((1, LANES), jnp.float32),
        ),
        in_specs=[
            pl.BlockSpec(memory_space=pltpu.HBM),
            pl.BlockSpec(memory_space=pltpu.HBM),
            pl.BlockSpec(memory_space=pltpu.HBM),
        ],
        out_specs=(vmem, vmem, vmem),
        scratch_shapes=[
            pltpu.VMEM(acts.shape, jnp.bfloat16),
            pltpu.VMEM((groups, tokens, columns), jnp.bfloat16),
            pltpu.VMEM((3 * tokens, tokens), jnp.bfloat16),
            pltpu.VMEM((tokens, columns), jnp.float32),
            pltpu.VMEM((most, tokens, LANES), jnp.float32),
            pltpu.VMEM((pair_count, 8, LANES), jnp.float32),
            pltpu.VMEM((16 if aligned else model, tokens), jnp.bfloat16),
            pltpu.VMEM((1, LANES), jnp.float32),
            pltpu.VMEM((total, 1, LANES), jnp.float32),
            dma((3,)),
            dma((groups, groups)),
            dma((groups,)),
            dma((groups, groups)),
            dma((groups, groups)),
            dma((groups, groups)),
            dma,
            dma,
            pltpu.SemaphoreType.REGULAR((max(1, (others - 1).bit_length()),)),
            pltpu.SMEM((groups,), jnp.int32),
        ],
        compiler_params=pltpu.CompilerParams(
            collective_id=0, has_side_effects=True, vmem_limit_bytes=VMEM_BYTES - kept
        ),
        name="mixer",
    )(order, acts, out_grads)
    update, weights = pl.pallas_call(
        expand,
        out_shape=(
            jax.ShapeDtypeStruct((part_rows, columns), jnp.float32),
            jax.ShapeDtypeStruct((groups,), jnp.float32),
        ),
        in_specs=[vmem, vmem, vmem],
        out_specs=(pl.BlockSpec(memory_space=pl.ANY), pl.BlockSpec(memory_space=pl.ANY)),
        scratch_shapes=[
            pltpu.VMEM((part_rows, columns), jnp.float32),
            pltpu.VMEM((groups,), jnp.float32),
            dma((pl.cdiv(part_rows, LANES),)),
            dma,
        ],
        compiler_params=pltpu.CompilerParams(vmem_limit_bytes=24 * 2**20),
        name="expand",
    )(acts_t, combined, weights_row)
    return (update, weights)


def solution(mesh):
    in_specs = (P(), P("task", None, "param"), P())
    out_specs = (P("task", "param"), P())
    return jax.shard_map(shards, mesh=mesh, in_specs=in_specs, out_specs=out_specs, check_vma=False)
```
